128 devices in a mesh: fsdp: 64 (over x_lo, y, z, core), grp: 2 (over x_hi).
Axes of the slice: x: 4 (x_hi: 2, x_lo: 2; x = x_hi * 2 + x_lo), y: 4, z: 4, core: 2. Of those that a mesh axis runs over, the one named last changes fastest.
Arguments:
- hidden: bfloat16 [32768, 3072], P('fsdp', 'grp'), may hold values from -16 to 16
- queries: bfloat16 [32768, 1536], P('fsdp', 'grp'), may hold values from -6 to 6
- attn_keys: bfloat16 [32768, 1536], P('fsdp', 'grp'), may hold values from -6 to 6
- w_value: bfloat16 [1536, 3072], P('fsdp', 'grp'), may hold values from -1 to 1
- w_out: bfloat16 [1536, 3072], P('fsdp', 'grp'), may hold values from -1 to 1
- alpha: float32 [3072], P('grp'), may hold values from 0.05 to 0.5
- out_grad: bfloat16 [32768, 3072], P('fsdp', 'grp'), may hold values from -6 to 6
Outputs:
- new_hidden: bfloat16 [32768, 3072], P('fsdp', 'grp')
- grad_hidden: bfloat16 [32768, 3072], P('fsdp', 'grp')
- grad_queries: bfloat16 [32768, 1536], P('fsdp', 'grp')
- grad_keys: bfloat16 [32768, 1536], P('fsdp', 'grp')
- grad_w_value: float32 [1536, 3072], P('fsdp', 'grp')
- grad_w_out: float32 [1536, 3072], P('fsdp', 'grp')
The draws below stay inside these ranges and needn't reach their ends.
All inputs are finite; a program needn't handle non-finite values.
Results may differ from the reference program's by a relative error of at most 0.012.
The reference program's roundings to bfloat16 on the way count: a program that leaves them out, or rounds other values in their place, can miss the bound.
Values may be sent and summed in bfloat16 or wider, within the bound.
No kernel may reach another device: no remote copies, remote signals or barrier semaphores. Data moves between devices by JAX's collectives and lax.ppermute only.
A program may use at most 192 MiB of HBM per device.

```python
import math
import jax
import jax.numpy as jnp
from jax import lax

D = 3072
HEADS = 12
HS = 128
SEQ = 512
HD = 1536
TOKENS = 32768


def column_scales(scale_key, width):
    position = jnp.arange(width, dtype=jnp.float32) / (width - 1)
    ramp_scale = jnp.exp(jnp.log(3.0) * (position - 0.5))
    roughness = jnp.exp(jax.random.uniform(scale_key, (width,), jnp.float32, -1.0, 1.0))
    return ramp_scale * roughness


def draw_hidden(key, part):
    row_key, col_key, val_key = jax.random.split(jax.random.fold_in(key, 5), 3)
    row_scale = jnp.exp(jax.random.uniform(row_key, (TOKENS, 1), jnp.float32, -1.15, 1.15))
    col_scale = column_scales(col_key, D)
    base_draw = jax.random.normal(val_key, (TOKENS, D), jnp.float32)
    return jnp.clip(base_draw * row_scale * col_scale, -16.0, 16.0).astype(jnp.bfloat16)


def weight_rows(key):
    row_key, col_key, val_key = jax.random.split(key, 3)
    row_scale = jnp.exp(jax.random.uniform(row_key, (HD, 1), jnp.float32, 0.0, jnp.log(10.0)))
    col_scale = column_scales(col_key, D)
    base_draw = jax.random.normal(val_key, (HD, D), jnp.float32)
    scaled = base_draw * row_scale * col_scale / (10.0 * D ** 0.5)
    return jnp.clip(scaled, -1.0, 1.0).astype(jnp.bfloat16)


def draw_w_value(key, part):
    return weight_rows(jax.random.fold_in(key, 11))


def draw_w_out(key, part):
    return weight_rows(jax.random.fold_in(key, 23))


def attention_pair(key):
    query_key, keys_key = jax.random.split(jax.random.fold_in(key, 37), 2)
    query_draw = jnp.clip(jax.random.normal(query_key, (TOKENS, HD), jnp.float32), -6.0, 6.0)
    keys_draw = jnp.clip(jax.random.normal(keys_key, (TOKENS, HD), jnp.float32), -6.0, 6.0)
    return (query_draw, keys_draw)


def draw_queries(key, part):
    return attention_pair(key)[0].astype(jnp.bfloat16)


def draw_attn_keys(key, part):
    return attention_pair(key)[1].astype(jnp.bfloat16)


def levels(own_key, shape, cuts, low, high):
    def one(dim, blocks):
        draws = jax.random.uniform(jax.random.fold_in(jax.random.fold_in(own_key, 6), dim), (blocks,), jnp.float32, low / len(cuts), high / len(cuts))
        return jnp.repeat(jnp.exp(draws), shape[dim] // blocks).reshape((-1,) + (1,) * (len(shape) - dim - 1))

    gain = one(*cuts[0])
    for cut in cuts[1:]:
        gain = gain * one(*cut)
    return gain


def gaussian(key, shape, scale, limit, shards=(), kind=jnp.bfloat16):
    loudness = levels(key, shape, shards, -0.22, 0.18) if shards else 1.0
    values = jax.random.normal(key, shape, jnp.float32) * scale * loudness
    return jnp.minimum(jnp.maximum(values, -limit), limit).astype(kind)


def setup_inputs(seed: int = 0) -> dict:
    seeds = jax.random.split(jax.random.key(seed), 8)
    hidden = draw_hidden(jax.random.fold_in(seeds[7], 71), 0)
    queries = draw_queries(jax.random.fold_in(seeds[7], 71), 0)
    attn_keys = draw_attn_keys(jax.random.fold_in(seeds[7], 71), 0)
    w_value = draw_w_value(jax.random.fold_in(seeds[7], 71), 0)
    w_out = draw_w_out(jax.random.fold_in(seeds[7], 71), 0)
    alpha = jnp.clip(jnp.exp(math.log(0.5) - 2.3025851 * jax.random.uniform(seeds[5], (D,), jnp.float32) ** levels(seeds[5], (D,), ((0, 2),), -0.2, 0.2)), 0.05, 0.5)
    out_grad = gaussian(seeds[6], (TOKENS, D), 1.0, 6.0, ((0, 64), (1, 2)))
    return dict(hidden=hidden, queries=queries, attn_keys=attn_keys, w_value=w_value, w_out=w_out, alpha=alpha, out_grad=out_grad)


EPS = 1e-06

def contract_last(left, right):
    return lax.dot_general(left, right, (((1,), (1,)), ((), ())), preferred_element_type=jnp.float32)

def contract_first(left, right):
    return lax.dot_general(left, right, (((0,), (0,)), ((), ())), preferred_element_type=jnp.float32)

def causal_probs(query_head, key_head):
    length = query_head.shape[0]
    score_scale = query_head.shape[1] ** (-0.5)
    scores = contract_last(query_head, key_head) * score_scale
    row_pos = lax.broadcasted_iota(jnp.int32, (length, length), 0)
    col_pos = lax.broadcasted_iota(jnp.int32, (length, length), 1)
    scores = jnp.where(row_pos >= col_pos, scores, -1e+30)
    row_peak = lax.optimization_barrier(jnp.max(scores, axis=1, keepdims=True))
    exp_terms = jnp.exp(scores - row_peak)
    return exp_terms / lax.optimization_barrier(jnp.sum(exp_terms, axis=1, keepdims=True))

def head_forward(items):
    query_head, key_head, value_head = items
    attn_prob = causal_probs(query_head, key_head)
    return jnp.dot(attn_prob.astype(jnp.bfloat16), value_head, preferred_element_type=jnp.float32).astype(jnp.bfloat16)

def head_backward(items):
    query_head, key_head, value_head, grad_head = items
    score_scale = query_head.shape[1] ** (-0.5)
    attn_prob = causal_probs(query_head, key_head)
    prob_half = attn_prob.astype(jnp.bfloat16)
    grad_prob = contract_last(grad_head, value_head)
    row_delta = lax.optimization_barrier(jnp.sum(attn_prob * grad_prob, axis=1, keepdims=True))
    grad_score = (attn_prob * (grad_prob - row_delta)).astype(jnp.bfloat16)
    grad_query = (jnp.dot(grad_score, key_head, preferred_element_type=jnp.float32) * score_scale).astype(jnp.bfloat16)
    grad_key = (contract_first(grad_score, query_head) * score_scale).astype(jnp.bfloat16)
    grad_value = contract_first(prob_half, grad_head).astype(jnp.bfloat16)
    return (grad_query, grad_key, grad_value)

def to_heads(block):
    return block.reshape(TOKENS // SEQ, SEQ, HEADS, HS).transpose(0, 2, 1, 3).reshape(-1, SEQ, HS)

def from_heads(stacked):
    return stacked.reshape(TOKENS // SEQ, HEADS, SEQ, HS).transpose(0, 2, 1, 3).reshape(TOKENS, HEADS * HS)

def unit_rows(weights):
    weights_f = weights.astype(jnp.float32)
    norms = jnp.sqrt(lax.optimization_barrier(jnp.sum(weights_f * weights_f, axis=1, keepdims=True)) + EPS)
    return (weights_f / norms, norms)

def unit_back(grad_unit, unit, norms):
    row_dot = lax.optimization_barrier(jnp.sum(grad_unit * unit, axis=1, keepdims=True))
    return (grad_unit - unit * row_dot) / norms

def reference(hidden, queries, attn_keys, w_value, w_out, alpha, out_grad):
    unit_v, norm_v = unit_rows(w_value)
    unit_o, norm_o = unit_rows(w_out)
    weight_v = unit_v.astype(jnp.bfloat16)
    weight_o = unit_o.astype(jnp.bfloat16)
    values = contract_last(hidden, weight_v).astype(jnp.bfloat16)
    q_heads = to_heads(queries)
    k_heads = to_heads(attn_keys)
    v_heads = to_heads(values)
    attn = from_heads(lax.map(head_forward, (q_heads, k_heads, v_heads)))
    proj = jnp.dot(attn, weight_o, preferred_element_type=jnp.float32)
    hidden_f = hidden.astype(jnp.float32)
    proj_rs = lax.rsqrt(lax.optimization_barrier(jnp.mean(proj * proj, axis=1, keepdims=True)) + EPS)
    mixed = hidden_f + alpha * (proj * proj_rs - hidden_f)
    mix_rs = lax.rsqrt(lax.optimization_barrier(jnp.mean(mixed * mixed, axis=1, keepdims=True)) + EPS)
    new_hidden = (mixed * mix_rs).astype(jnp.bfloat16)
    grad_out = out_grad.astype(jnp.float32)
    grad_mix = mix_rs * (grad_out - mixed * mix_rs * mix_rs * lax.optimization_barrier(jnp.mean(grad_out * mixed, axis=1, keepdims=True)))
    grad_res = grad_mix * (1.0 - alpha)
    grad_pn = grad_mix * alpha
    grad_proj = proj_rs * (grad_pn - proj * proj_rs * proj_rs * lax.optimization_barrier(jnp.mean(grad_pn * proj, axis=1, keepdims=True)))
    grad_proj_b = grad_proj.astype(jnp.bfloat16)
    grad_attn = contract_last(grad_proj_b, weight_o).astype(jnp.bfloat16)
    gw_o = contract_first(attn, grad_proj_b)
    grad_q, grad_k, grad_v = lax.map(head_backward, (q_heads, k_heads, v_heads, to_heads(grad_attn)))
    grad_values = from_heads(grad_v)
    grad_hidden = (grad_res + jnp.dot(grad_values, weight_v, preferred_element_type=jnp.float32)).astype(jnp.bfloat16)
    gw_v = contract_first(grad_values, hidden)
    grad_w_value = unit_back(gw_v, unit_v, norm_v)
    grad_w_out = unit_back(gw_o, unit_o, norm_o)
    return (new_hidden, grad_hidden, from_heads(grad_q), from_heads(grad_k), grad_w_value, grad_w_out)
```

```python
import jax
import jax.numpy as jnp
from jax import lax
from jax.experimental import pallas as pl
from jax.experimental.pallas import tpu as pltpu
from jax.sharding import Mesh
from jax.sharding import PartitionSpec as P

D = 3072
HS = 128
X, Y, Z, C, G = "fsdp_0", "fsdp_1", "fsdp_2", "fsdp_3", "grp"
FSDP = (X, Y, Z, C)
YZ = (Y, Z)
EPS = 1e-06
SWAP = [(0, 1), (1, 0)]
F32 = jnp.float32
BF16 = jnp.bfloat16


def contract_last(left, right):
    return lax.dot_general(left, right, (((1,), (1,)), ((), ())), preferred_element_type=F32)


def contract_first(left, right):
    return lax.dot_general(left, right, (((0,), (0,)), ((), ())), preferred_element_type=F32)


def matmul(left, right):
    return jnp.dot(left, right, preferred_element_type=F32)


def probs_kernel(q_ref, k_ref, p_ref):
    length = q_ref.shape[0]
    scores = contract_last(q_ref[...], k_ref[...]) * (HS**-0.5)
    row_pos = lax.broadcasted_iota(jnp.int32, (length, length), 0)
    col_pos = lax.broadcasted_iota(jnp.int32, (length, length), 1)
    scores = jnp.where(row_pos >= col_pos, scores, -1e30)
    terms = jnp.exp(scores - jnp.max(scores, axis=1, keepdims=True))
    p_ref[0] = terms * (1.0 / jnp.sum(terms, axis=1, keepdims=True))


def forward_kernel(p_ref, own_ref, peer_ref, v_ref, attn_ref):
    value = (own_ref[...] + peer_ref[...].astype(F32)).astype(BF16)
    v_ref[...] = value
    attn_ref[...] = matmul(p_ref[0].astype(BF16), value).astype(BF16)


def backward_kernel(q_ref, k_ref, v_ref, p_ref, own_ref, peer_ref, dq_ref, dk_ref, dv_ref):
    scale = HS**-0.5
    prob = p_ref[0]
    grad = (own_ref[...] + peer_ref[...].astype(F32)).astype(BF16)
    grad_prob = contract_last(grad, v_ref[...])
    delta = jnp.sum(prob * grad_prob, axis=1, keepdims=True)
    grad_score = (prob * (grad_prob - delta)).astype(BF16)
    dv_ref[...] = contract_first(prob.astype(BF16), grad).astype(BF16)
    dq_ref[...] = (matmul(grad_score, k_ref[...]) * scale).astype(BF16)
    dk_ref[...] = (contract_first(grad_score, q_ref[...]) * scale).astype(BF16)


def heads_call(kernel, name, operands, tokens, width, results, probs_out=False):
    heads = width // HS
    slab = pl.BlockSpec((tokens, HS), lambda h: (0, h))
    square = pl.BlockSpec((1, tokens, tokens), lambda h: (h, 0, 0))
    if probs_out:
        shapes = jax.ShapeDtypeStruct((heads, tokens, tokens), F32)
        specs = square
    else:
        shapes = [jax.ShapeDtypeStruct((tokens, width), BF16)] * results
        specs = [slab] * results
    dots = 1 if probs_out else (1 if results == 2 else 4)
    return pl.pallas_call(
        kernel,
        grid=(heads,),
        in_specs=[square if o.ndim == 3 else slab for o in operands],
        out_specs=specs,
        out_shape=shapes,
        name=name,
        cost_estimate=pl.CostEstimate(
            flops=2 * dots * heads * tokens * tokens * HS * 2,
            bytes_accessed=heads * tokens * (tokens * 4 + HS * 10),
            transcendentals=heads * tokens * tokens if probs_out else 0,
        ),
        compiler_params=pltpu.CompilerParams(dimension_semantics=("arbitrary",)),
    )(*operands)


def ordered(me, mine, other, axis=0):
    return jnp.where(
        me == 0, jnp.stack([mine, other], axis), jnp.stack([other, mine], axis)
    )


def row_block(weights, index):
    rows = weights.shape[0] // 2
    return lax.dynamic_slice_in_dim(weights, index * rows, rows, 0)


def gather_rows(pair):
    planes = lax.axis_size(Y) * lax.axis_size(Z)
    core = lax.axis_index(C)
    got = lax.all_to_all(
        jnp.broadcast_to(pair[None], (planes, *pair.shape)), YZ, 0, 0, tiled=True
    )
    other = lax.ppermute(got, C, SWAP)
    both = ordered(core, got.swapaxes(0, 1), other.swapaxes(0, 1), axis=2)
    return both.reshape(-1, pair.shape[-1])


def summed_rows(grads, blocks):
    planes = lax.axis_size(Y) * lax.axis_size(Z)
    core = lax.axis_index(C)
    width = grads.shape[-1]
    parts = grads.reshape(blocks, planes, 2, -1, width)
    send = lax.dynamic_index_in_dim(parts, 1 - core, 2, keepdims=False).astype(BF16)
    keep = lax.dynamic_index_in_dim(parts, core, 2, keepdims=False)
    chip = (keep + lax.ppermute(send, C, SWAP).astype(F32)).astype(BF16)
    arrived = lax.all_to_all(chip.swapaxes(0, 1), YZ, 0, 0, tiled=True)
    return jnp.sum(arrived.astype(F32), axis=0)


def onto_owner(first, second, side):
    send = jnp.where(side == 0, second, first)
    keep = jnp.where(side == 0, first, second)
    return keep + lax.ppermute(send, X, SWAP)


def shards(hidden, queries, attn_keys, w_value, w_out, alpha, out_grad):
    half_width = hidden.shape[1]
    rows = w_value.shape[0]
    tokens, width = queries.shape
    side, grp = lax.axis_index(X), lax.axis_index(G)

    both_w = jnp.concatenate((w_value, w_out), axis=0)
    next_w = lax.ppermute(both_w, X, SWAP)
    own_f, next_f = both_w.astype(F32), next_w.astype(F32)
    own_part = jnp.sum(own_f * own_f, axis=1)
    next_part = jnp.sum(next_f * next_f, axis=1)
    own_sq = own_part + lax.ppermute(own_part, G, SWAP)
    next_sq = next_part + lax.ppermute(own_part, (X, G), [(0, 3), (1, 2), (2, 1), (3, 0)])
    own_norm = jnp.sqrt(own_sq + EPS)[:, None]
    next_norm = jnp.sqrt(next_sq + EPS)[:, None]
    own_unit = own_f / own_norm
    own_unit_b = own_unit.astype(BF16)
    next_unit_b = (next_f / next_norm).astype(BF16)
    weight_v = gather_rows(ordered(side, own_unit_b[:rows], next_unit_b[:rows]))
    weight_o = gather_rows(ordered(side, own_unit_b[rows:], next_unit_b[rows:]))

    probs = heads_call(probs_kernel, "probs", (queries, attn_keys), tokens, width, 1, True)
    value_send = contract_last(hidden, row_block(weight_v, 1 - grp)).astype(BF16)
    value_peer = lax.ppermute(value_send, G, SWAP)
    value_own = contract_last(hidden, row_block(weight_v, grp))
    values, attn = heads_call(
        forward_kernel, "forward", (probs, value_own, value_peer), tokens, width, 2
    )
    attn_peer = lax.ppermute(attn, G, SWAP)

    proj = matmul(attn, row_block(weight_o, grp)) + matmul(attn_peer, row_block(weight_o, 1 - grp))
    hidden_f = hidden.astype(F32)
    grad_out = out_grad.astype(F32)
    keep_rate = 1.0 - alpha
    moments = jnp.stack(
        (
            jnp.sum(proj * proj, axis=1),
            jnp.sum(keep_rate * keep_rate * hidden_f * hidden_f, axis=1),
            jnp.sum(keep_rate * alpha * hidden_f * proj, axis=1),
            jnp.sum(alpha * alpha * proj * proj, axis=1),
            jnp.sum(grad_out * keep_rate * hidden_f, axis=1),
            jnp.sum(grad_out * alpha * proj, axis=1),
        )
    )
    moments = moments + lax.ppermute(moments, G, SWAP)
    proj_rs = lax.rsqrt(moments[0] / D + EPS)[:, None]
    cross_sum = moments[2][:, None]
    alpha_sum = moments[3][:, None]
    mix_mean = (moments[1][:, None] + 2.0 * proj_rs * cross_sum + proj_rs * proj_rs * alpha_sum) / D
    mix_rs = lax.rsqrt(mix_mean + EPS)
    mixed = hidden_f + alpha * (proj * proj_rs - hidden_f)
    new_hidden = (mixed * mix_rs).astype(BF16)
    grad_mean = (moments[4][:, None] + proj_rs * moments[5][:, None]) / D
    grad_mix = mix_rs * (grad_out - mixed * mix_rs * mix_rs * grad_mean)
    grad_pn = grad_mix * alpha
    proj_mean = (
        mix_rs * moments[5][:, None]
        - mix_rs * mix_rs * mix_rs * grad_mean * (cross_sum + proj_rs * alpha_sum)
    ) / D
    grad_res = grad_mix * keep_rate
    grad_proj = proj_rs * (grad_pn - proj * proj_rs * proj_rs * proj_mean)
    grad_proj_b = grad_proj.astype(BF16)

    grad_send = contract_last(grad_proj_b, row_block(weight_o, 1 - grp)).astype(BF16)
    grad_peer = lax.ppermute(grad_send, G, SWAP)
    grad_own = contract_last(grad_proj_b, row_block(weight_o, grp))
    attn_all = jnp.where(
        grp == 0,
        jnp.concatenate((attn, attn_peer), axis=1),
        jnp.concatenate((attn_peer, attn), axis=1),
    )
    gw_o = summed_rows(contract_first(attn_all, grad_proj_b), 2)
    grad_q, grad_k, grad_v = heads_call(
        backward_kernel,
        "backward",
        (queries, attn_keys, values, probs, grad_own, grad_peer),
        tokens,
        width,
        3,
    )
    grad_v_peer = lax.ppermute(grad_v, G, SWAP)

    grad_hidden = (
        grad_res
        + matmul(grad_v, row_block(weight_v, grp))
        + matmul(grad_v_peer, row_block(weight_v, 1 - grp))
    ).astype(BF16)
    gw_v_own = summed_rows(contract_first(grad_v, hidden), 1)[0]
    gw_v_peer = summed_rows(contract_first(grad_v_peer, hidden), 1)[0]
    gw_o_mine = onto_owner(gw_o[0], gw_o[1], side)
    gw_v_mine = onto_owner(
        jnp.where(grp == 0, gw_v_own, gw_v_peer), jnp.where(grp == 0, gw_v_peer, gw_v_own), side
    )
    unit_v, unit_o = own_unit[:rows], own_unit[rows:]
    dots = jnp.stack((jnp.sum(gw_v_mine * unit_v, axis=1), jnp.sum(gw_o_mine * unit_o, axis=1)))
    dots = dots + lax.ppermute(dots, G, SWAP)
    grad_w_value = (gw_v_mine - unit_v * dots[0][:, None]) / own_norm[:rows]
    grad_w_out = (gw_o_mine - unit_o * dots[1][:, None]) / own_norm[rows:]
    return new_hidden, grad_hidden, grad_q, grad_k, grad_w_value, grad_w_out


def solution(mesh):
    torus = Mesh(mesh.devices.reshape(2, 4, 4, 2, mesh.shape[G]), (*FSDP, G))
    placed = P(FSDP, G)
    return jax.shard_map(
        shards,
        mesh=torus,
        in_specs=(placed,) * 5 + (P(G), placed),
        out_specs=(placed,) * 6,
        check_vma=False,
    )
```

```python
import jax
import jax.numpy as jnp
from jax import lax
from jax.experimental import pallas as pl
from jax.experimental.pallas import tpu as pltpu
from jax.sharding import Mesh
from jax.sharding import PartitionSpec as P


D = 3072
HS = 128
X, Y, Z, C, G = "fsdp_0", "fsdp_1", "fsdp_2", "fsdp_3", "grp"
FSDP = (X, Y, Z, C)
YZ = (Y, Z)
EPS = 1e-06
SWAP = [(0, 1), (1, 0)]
ACROSS = [(0, 3), (1, 2), (2, 1), (3, 0)]
F32 = jnp.float32
BF16 = jnp.bfloat16


def contract_last(left, right):
    return lax.dot_general(left, right, (((1,), (1,)), ((), ())), preferred_element_type=F32)


def contract_first(left, right):
    return lax.dot_general(left, right, (((0,), (0,)), ((), ())), preferred_element_type=F32)


def matmul(left, right):
    return jnp.dot(left, right, preferred_element_type=F32)


def probs_kernel(q_ref, k_ref, p_ref):
    length = q_ref.shape[0]
    scores = contract_last(q_ref[...], k_ref[...]) * (HS**-0.5)
    row_pos = lax.broadcasted_iota(jnp.int32, (length, length), 0)
    col_pos = lax.broadcasted_iota(jnp.int32, (length, length), 1)
    scores = jnp.where(row_pos >= col_pos, scores, -1e30)
    terms = jnp.exp(scores - jnp.max(scores, axis=1, keepdims=True))
    p_ref[0] = terms * (1.0 / jnp.sum(terms, axis=1, keepdims=True))


def forward_kernel(p_ref, own_ref, peer_ref, rate_ref, v_ref, attn_ref):
    value = ((own_ref[...] + peer_ref[...].astype(F32)) * rate_ref[0:1, :]).astype(BF16)
    v_ref[...] = value
    attn_ref[...] = matmul(p_ref[0].astype(BF16), value).astype(BF16)


def backward_kernel(q_ref, k_ref, v_ref, p_ref, own_ref, peer_ref, dq_ref, dk_ref, dv_ref):
    scale = HS**-0.5
    prob = p_ref[0]
    grad = (own_ref[...] + peer_ref[...].astype(F32)).astype(BF16)
    grad_prob = contract_last(grad, v_ref[...])
    delta = jnp.sum(prob * grad_prob, axis=1, keepdims=True)
    grad_score = (prob * (grad_prob - delta)).astype(BF16)
    dv_ref[...] = contract_first(prob.astype(BF16), grad).astype(BF16)
    dq_ref[...] = (matmul(grad_score, k_ref[...]) * scale).astype(BF16)
    dk_ref[...] = (contract_first(grad_score, q_ref[...]) * scale).astype(BF16)


def heads_call(kernel, heads, operands, results, dots):
    def spec(shape, first):
        if len(shape) == 3:
            return pl.BlockSpec((1, *shape[1:]), lambda h: (first + h, 0, 0))
        return pl.BlockSpec((shape[0], HS), lambda h: (0, first + h))

    tokens = operands[0][0].shape[-2]
    return pl.pallas_call(
        kernel,
        grid=(heads,),
        in_specs=[spec(o.shape, first) for o, first in operands],
        out_specs=[spec(shape, first) for shape, _, first in results],
        out_shape=[jax.ShapeDtypeStruct(shape, dtype) for shape, dtype, _ in results],
        cost_estimate=pl.CostEstimate(
            flops=4 * dots * heads * tokens * tokens * HS,
            bytes_accessed=heads * tokens * (tokens * 4 + HS * 10),
            transcendentals=0,
        ),
        compiler_params=pltpu.CompilerParams(dimension_semantics=("arbitrary",)),
    )(*[o for o, _ in operands])


def exchanged(value, axis=G):
    return lax.ppermute(value, axis, SWAP)


def chosen(first_if, first, second):
    return jnp.where(first_if, first, second)


def columns(value, index):
    half = value.shape[-1] // 2
    return jnp.where(index == 0, value[..., :half], value[..., half:])


def in_order(index, mine, other, axis):
    return jnp.where(
        index == 0,
        jnp.concatenate([mine, other], axis),
        jnp.concatenate([other, mine], axis),
    )


def over_planes(rows):
    planes = lax.axis_size(Y) * lax.axis_size(Z)
    got = lax.all_to_all(jnp.broadcast_to(rows[None], (planes, *rows.shape)), YZ, 0, 0, tiled=True)
    return got.swapaxes(0, 1) if rows.ndim == 3 else got.reshape(-1, rows.shape[-1])


def product_kernel(*refs):
    *lefts, near_ref, other_ref, out_ref = refs
    runs, _, each, width = out_ref.shape
    for i in range(len(lefts) // 2):
        total = contract_first(lefts[2 * i][...], near_ref[...])
        total = total + contract_first(lefts[2 * i + 1][...], other_ref[...])
        out_ref[:, i] = total.astype(BF16).reshape(runs, each, width)


def products(lefts, near, other, each, steps=2):
    tokens, count = lefts[0].shape
    width = near.shape[1]
    block = count // steps
    pairs = len(lefts) // 2
    return pl.pallas_call(
        product_kernel,
        grid=(steps,),
        in_specs=[pl.BlockSpec((tokens, block), lambda i: (0, i))] * len(lefts)
        + [pl.BlockSpec((tokens, width), lambda i: (0, 0))] * 2,
        out_specs=pl.BlockSpec((block // each, pairs, each, width), lambda i: (i, 0, 0, 0)),
        out_shape=jax.ShapeDtypeStruct((count // each, pairs, each, width), BF16),
        cost_estimate=pl.CostEstimate(
            flops=2 * tokens * count * width * len(lefts),
            bytes_accessed=4 * count * width,
            transcendentals=0,
        ),
        compiler_params=pltpu.CompilerParams(dimension_semantics=("arbitrary",)),
    )(*lefts, near, other)


def arriving(tiles, after=None):
    if after is not None:
        tiles, _ = lax.optimization_barrier((tiles, after))
    return lax.all_to_all(tiles, YZ, 0, 0, tiled=True)


def summed(arrived):
    return jnp.sum(arrived.astype(F32), axis=0)


def owned(own, peer, at_own, core, unit):
    keep, send = chosen(at_own, own, peer), chosen(at_own, peer, own)
    count = keep.shape[0] // 2

    def part(value, index):
        return chosen(index == 0, value[:count], value[count:])

    far = lax.ppermute(part(send, 1 - core), (X, C), ACROSS)
    near = part(keep, core) + exchanged(part(send, core), X)
    far = far + exchanged(part(keep, 1 - core), C)
    rows = in_order(core, near, far, 1)
    dots = jnp.sum(rows * unit, axis=1)
    return rows, (dots + exchanged(dots))[:, None]


def shards(hidden, queries, attn_keys, w_value, w_out, alpha, out_grad):
    rows = w_value.shape[0]
    tokens, width = queries.shape
    heads = width // HS
    side, core, grp = lax.axis_index(X), lax.axis_index(C), lax.axis_index(G)
    at_own = side == grp

    next_v = exchanged(w_value, X)
    pair_v = jnp.stack((chosen(at_own, next_v, w_value), chosen(at_own, w_value, next_v)))
    other_v = exchanged(columns(pair_v, 1 - core), C)
    pair_v = in_order(core, columns(pair_v, core), other_v, 1)
    raw_near = over_planes(pair_v)
    raw_far = exchanged(raw_near, C)
    raw_near, raw_far = (w.reshape(2, width, -1) for w in (raw_near, raw_far))

    next_o = exchanged(w_out, X)
    own_vf, own_of = w_value.astype(F32), w_out.astype(F32)
    next_of = next_o.astype(F32)
    own_part = jnp.stack((jnp.sum(own_of * own_of, axis=1), jnp.sum(own_vf * own_vf, axis=1)))
    next_part = jnp.sum(next_of * next_of, axis=1)
    own_sq = own_part + lax.ppermute(own_part, G, SWAP)
    next_sq = next_part + lax.ppermute(own_part[0], (X, G), ACROSS)
    norm_o, norm_v = jnp.sqrt(own_sq[0] + EPS)[:, None], jnp.sqrt(own_sq[1] + EPS)[:, None]
    unit_v, unit_o = own_vf / norm_v, own_of / norm_o
    here = unit_o.astype(BF16)
    there = (next_of / jnp.sqrt(next_sq + EPS)[:, None]).astype(BF16)
    pair_o = jnp.stack((chosen(at_own, here, there), chosen(at_own, there, here)))
    send_o = columns(pair_o, 1 - core)
    other_o = exchanged(send_o, C)
    pair_o = in_order(core, columns(pair_o, core), other_o, 1)
    pair_o, _ = lax.optimization_barrier((pair_o, raw_near))
    both_o = over_planes(pair_o)
    both_o_far = exchanged(both_o, C)
    weight_o = in_order(core, both_o, both_o_far, 3)
    weight_o = weight_o.reshape(2, width, -1)
    weight_o_own, weight_o_peer = weight_o[0], weight_o[1]

    (probs,) = heads_call(
        probs_kernel, heads, ((queries, 0), (attn_keys, 0)), (((heads, tokens, tokens), F32, 0),), 1
    )
    hidden_near, hidden_far = lax.optimization_barrier(
        (columns(hidden, core), columns(hidden, 1 - core))
    )
    hidden_other = exchanged(hidden_far, C)
    full = (tokens, width)
    part = contract_last(hidden_near, raw_near[0]) + contract_last(hidden_far, raw_far[0])
    part = part.astype(BF16)
    value_peer = exchanged(part)
    value_own = contract_last(hidden_near, raw_near[1]) + contract_last(hidden_far, raw_far[1])
    near, far, _ = lax.optimization_barrier((raw_near, raw_far, part))
    half_sq = jnp.sum(jnp.square(near.astype(F32)), axis=2)
    half_sq = half_sq + jnp.sum(jnp.square(far.astype(F32)), axis=2)
    all_sq = half_sq + exchanged(half_sq)[::-1]
    own_rate = jnp.broadcast_to(lax.rsqrt(all_sq[1] + EPS)[None], (8, width))
    values, attn_own = heads_call(
        forward_kernel,
        heads,
        ((probs, 0), (value_own, 0), (value_peer, 0), (own_rate, 0)),
        ((full, BF16, 0), (full, BF16, 0)),
        1,
    )
    attn_their = exchanged(attn_own)
    weight_v = in_order(core, near, far, 2).astype(F32) / jnp.sqrt(all_sq + EPS)[..., None]
    weight_v_peer, weight_v_own = weight_v[0].astype(BF16), weight_v[1].astype(BF16)

    attn_own_other = exchanged(attn_own, C)
    proj = lax.optimization_barrier(matmul(attn_own, weight_o_own))
    attn_their_other = exchanged(attn_their, C)
    proj = proj + matmul(attn_their, weight_o_peer)
    hidden_f = hidden.astype(F32)
    grad_out = out_grad.astype(F32)
    keep_rate = 1.0 - alpha
    moments = jnp.stack(
        (
            jnp.sum(proj * proj, axis=1),
            jnp.sum(keep_rate * keep_rate * hidden_f * hidden_f, axis=1),
            jnp.sum(keep_rate * alpha * hidden_f * proj, axis=1),
            jnp.sum(alpha * alpha * proj * proj, axis=1),
            jnp.sum(grad_out * keep_rate * hidden_f, axis=1),
            jnp.sum(grad_out * alpha * proj, axis=1),
        )
    )
    moments = moments + exchanged(moments)
    proj_rs = lax.rsqrt(moments[0] / D + EPS)[:, None]
    cross_sum = moments[2][:, None]
    alpha_sum = moments[3][:, None]
    mix_mean = (moments[1][:, None] + 2.0 * proj_rs * cross_sum + proj_rs * proj_rs * alpha_sum) / D
    mix_rs = lax.rsqrt(mix_mean + EPS)
    mixed = hidden_f + alpha * (proj * proj_rs - hidden_f)
    new_hidden = (mixed * mix_rs).astype(BF16)
    grad_mean = (moments[4][:, None] + proj_rs * moments[5][:, None]) / D
    grad_mix = mix_rs * (grad_out - mixed * mix_rs * mix_rs * grad_mean)
    grad_pn = grad_mix * alpha
    proj_mean = (
        mix_rs * moments[5][:, None]
        - mix_rs * mix_rs * mix_rs * grad_mean * (cross_sum + proj_rs * alpha_sum)
    ) / D
    grad_res = grad_mix * keep_rate
    grad_proj = proj_rs * (grad_pn - proj * proj_rs * proj_rs * proj_mean)
    grad_proj_b = grad_proj.astype(BF16)

    grad_near, grad_far = lax.optimization_barrier(
        (columns(grad_proj_b, core), columns(grad_proj_b, 1 - core))
    )
    grad_other = exchanged(grad_far, C)
    part = contract_last(grad_proj_b, weight_o_peer).astype(BF16)
    grad_peer = exchanged(part)
    grad_own = contract_last(grad_proj_b, weight_o_own)
    lefts = (attn_own, attn_own_other, attn_their, attn_their_other)
    at_o = arriving(products(lefts, grad_near, grad_other, 2 * rows))
    gw_o = summed(at_o)
    grad_q, grad_k, gv_own = heads_call(
        backward_kernel,
        heads,
        tuple((o, 0) for o in (queries, attn_keys, values, probs, grad_own, grad_peer)),
        ((full, BF16, 0),) * 3,
        4,
    )
    gv_peer = exchanged(gv_own)

    gv_own_other = exchanged(gv_own, C)
    tiles = products((gv_own, gv_own_other), hidden_near, hidden_other, 2 * rows)
    at_own_v = arriving(tiles, at_o)
    gw_v_own = summed(at_own_v)[0]
    gv_peer_other = exchanged(gv_peer, C)
    tiles = products((gv_peer, gv_peer_other), hidden_near, hidden_other, 2 * rows)
    gw_v_peer = summed(arriving(tiles, at_own_v))[0]
    from_own = lax.optimization_barrier(matmul(gv_own, weight_v_own))
    from_peer = matmul(gv_peer, weight_v_peer)
    grad_hidden = (grad_res + from_own + from_peer).astype(BF16)
    gw_o_mine, dot_o = owned(gw_o[0], gw_o[1], at_own, core, unit_o)
    gw_v_mine, dot_v = owned(gw_v_own, gw_v_peer, at_own, core, unit_v)
    grad_w_value = (gw_v_mine - unit_v * dot_v) / norm_v
    grad_w_out = (gw_o_mine - unit_o * dot_o) / norm_o
    return new_hidden, grad_hidden, grad_q, grad_k, grad_w_value, grad_w_out


def solution(mesh):
    torus = Mesh(mesh.devices.reshape(2, 4, 4, 2, mesh.shape[G]), (*FSDP, G))
    placed = P(FSDP, G)
    return jax.shard_map(
        shards,
        mesh=torus,
        in_specs=(placed,) * 5 + (P(G), placed),
        out_specs=(placed,) * 6,
        check_vma=False,
    )
```

```python
import functools

import jax
import jax.numpy as jnp
from jax import lax
from jax.experimental import pallas as pl
from jax.experimental.pallas import tpu as pltpu
from jax.sharding import Mesh
from jax.sharding import PartitionSpec as P


D = 3072
HS = 128
X, Y, Z, C, G = "fsdp_0", "fsdp_1", "fsdp_2", "fsdp_3", "grp"
FSDP = (X, Y, Z, C)
YZ = (Y, Z)
EPS = 1e-06
SWAP = [(0, 1), (1, 0)]
ACROSS = [(0, 3), (1, 2), (2, 1), (3, 0)]
F32 = jnp.float32
BF16 = jnp.bfloat16


def contract_last(left, right):
    return lax.dot_general(left, right, (((1,), (1,)), ((), ())), preferred_element_type=F32)


def contract_first(left, right):
    return lax.dot_general(left, right, (((0,), (0,)), ((), ())), preferred_element_type=F32)


def matmul(left, right):
    return jnp.dot(left, right, preferred_element_type=F32)


def probs_kernel(q_ref, k_ref, p_ref):
    length = q_ref.shape[0]
    scores = contract_last(q_ref[...], k_ref[...]) * (HS**-0.5)
    row_pos = lax.broadcasted_iota(jnp.int32, (length, length), 0)
    col_pos = lax.broadcasted_iota(jnp.int32, (length, length), 1)
    scores = jnp.where(row_pos >= col_pos, scores, -1e30)
    terms = jnp.exp(scores - jnp.max(scores, axis=1, keepdims=True))
    p_ref[0] = terms * (1.0 / jnp.sum(terms, axis=1, keepdims=True))


def forward_kernel(p_ref, own_ref, peer_ref, rate_ref, v_ref, attn_ref):
    value = ((own_ref[...] + peer_ref[...].astype(F32)) * rate_ref[0:1, :]).astype(BF16)
    v_ref[...] = value
    attn_ref[...] = matmul(p_ref[0].astype(BF16), value).astype(BF16)


def backward_kernel(q_ref, k_ref, v_ref, p_ref, own_ref, peer_ref, dq_ref, dk_ref, dv_ref):
    scale = HS**-0.5
    prob = p_ref[0]
    grad = (own_ref[...] + peer_ref[...].astype(F32)).astype(BF16)
    grad_prob = contract_last(grad, v_ref[...])
    delta = jnp.sum(prob * grad_prob, axis=1, keepdims=True)
    grad_score = (prob * (grad_prob - delta)).astype(BF16)
    dv_ref[...] = contract_first(prob.astype(BF16), grad).astype(BF16)
    dq_ref[...] = (matmul(grad_score, k_ref[...]) * scale).astype(BF16)
    dk_ref[...] = (contract_first(grad_score, q_ref[...]) * scale).astype(BF16)


def heads_call(kernel, heads, operands, results, dots):
    def spec(shape, first):
        if len(shape) == 3:
            return pl.BlockSpec((1, *shape[1:]), lambda h: (first + h, 0, 0))
        return pl.BlockSpec((shape[0], HS), lambda h: (0, first + h))

    tokens = operands[0][0].shape[-2]
    return pl.pallas_call(
        kernel,
        grid=(heads,),
        in_specs=[spec(o.shape, first) for o, first in operands],
        out_specs=[spec(shape, first) for shape, _, first in results],
        out_shape=[jax.ShapeDtypeStruct(shape, dtype) for shape, dtype, _ in results],
        cost_estimate=pl.CostEstimate(
            flops=4 * dots * heads * tokens * tokens * HS,
            bytes_accessed=heads * tokens * (tokens * 4 + HS * 10),
            transcendentals=0,
        ),
        compiler_params=pltpu.CompilerParams(dimension_semantics=("arbitrary",)),
    )(*[o for o, _ in operands])


def exchanged(value, axis=G):
    return lax.ppermute(value, axis, SWAP)


def chosen(first_if, first, second):
    return jnp.where(first_if, first, second)


def columns(value, index):
    half = value.shape[-1] // 2
    return jnp.where(index == 0, value[..., :half], value[..., half:])


def in_order(index, mine, other, axis):
    return jnp.where(
        index == 0,
        jnp.concatenate([mine, other], axis),
        jnp.concatenate([other, mine], axis),
    )


def over_planes(rows):
    planes = lax.axis_size(Y) * lax.axis_size(Z)
    got = lax.all_to_all(jnp.broadcast_to(rows[None], (planes, *rows.shape)), YZ, 0, 0, tiled=True)
    return got.swapaxes(0, 1) if rows.ndim == 3 else got.reshape(-1, rows.shape[-1])


def shifted(value, axis, step):
    count = lax.axis_size(axis)
    return lax.ppermute(value, axis, [(i, (i + step) % count) for i in range(count)])


def spread(rows):
    ny, nz = lax.axis_size(Y), lax.axis_size(Z)
    half = rows.shape[-1] // 2
    left, right = rows[..., :half], rows[..., half:]
    left = jnp.stack([left] + [shifted(left, Y, k) for k in range(1, ny)])
    right = jnp.stack([right] + [shifted(right, Z, k) for k in range(1, nz)])
    lefts = [left] + [shifted(left, Z, k) for k in range(1, nz)]
    rights = [right] + [shifted(right, Y, k) for k in range(1, ny)]
    return lefts, rights


def placed_kernel(place_ref, *refs, ny, nz):
    *pieces, near_ref, far_ref, near_rows, far_rows, part_ref = refs
    each, half = pieces[0].shape[2:]
    y, z = place_ref[0], place_ref[1]

    def run(plane_y, plane_z):
        return pl.ds(pl.multiple_of((plane_y * nz + plane_z) * each, each), each)

    for group, rows_ref in ((0, near_rows), (ny + nz, far_rows)):
        for ky in range(ny):
            for kz in range(nz):
                at = run(lax.rem(y + ny - ky, ny), lax.rem(z + nz - kz, nz))
                for block in range(2):
                    rows_ref[block, at, :half] = pieces[group + kz][ky, block]
                    rows_ref[block, at, half:] = pieces[group + nz + ky][kz, block]
    step = near_ref.shape[0] // 2

    @pl.loop(0, 2)
    def _(i):
        at = pl.ds(pl.multiple_of(i * step, step), step)
        part = contract_last(near_ref[at, :], near_rows[0])
        part = part + contract_last(far_ref[at, :], far_rows[0])
        part_ref[at, :] = part.astype(BF16)


def placed(near, far, hidden_near, hidden_far):
    nz, ny = len(near[0]), len(near[1])
    pieces = (*near[0], *near[1], *far[0], *far[1])
    each, half = pieces[0].shape[2:]
    count = ny * nz * each
    tokens = hidden_near.shape[0]
    place = jnp.stack((lax.axis_index(Y), lax.axis_index(Z))).astype(jnp.int32)
    vmem = pl.BlockSpec(memory_space=pltpu.VMEM)
    rows = jax.ShapeDtypeStruct((2, count, 2 * half), BF16)
    return pl.pallas_call(
        functools.partial(placed_kernel, ny=ny, nz=nz),
        in_specs=[pl.BlockSpec(memory_space=pltpu.SMEM)] + [vmem] * (len(pieces) + 2),
        out_specs=[vmem] * 3,
        out_shape=[rows, rows, jax.ShapeDtypeStruct((tokens, count), BF16)],
        cost_estimate=pl.CostEstimate(
            flops=8 * tokens * count * half, bytes_accessed=16 * count * half, transcendentals=0
        ),
    )(place, *pieces, hidden_near, hidden_far)


def product_kernel(*refs):
    *lefts, near_ref, other_ref, out_ref = refs
    runs, _, each, width = out_ref.shape
    for i in range(len(lefts) // 2):
        total = contract_first(lefts[2 * i][...], near_ref[...])
        total = total + contract_first(lefts[2 * i + 1][...], other_ref[...])
        out_ref[:, i] = total.astype(BF16).reshape(runs, each, width)


def products(lefts, near, other, each, steps=2):
    tokens, count = lefts[0].shape
    width = near.shape[1]
    block = count // steps
    pairs = len(lefts) // 2
    return pl.pallas_call(
        product_kernel,
        grid=(steps,),
        in_specs=[pl.BlockSpec((tokens, block), lambda i: (0, i))] * len(lefts)
        + [pl.BlockSpec((tokens, width), lambda i: (0, 0))] * 2,
        out_specs=pl.BlockSpec((block // each, pairs, each, width), lambda i: (i, 0, 0, 0)),
        out_shape=jax.ShapeDtypeStruct((count // each, pairs, each, width), BF16),
        cost_estimate=pl.CostEstimate(
            flops=2 * tokens * count * width * len(lefts),
            bytes_accessed=4 * count * width,
            transcendentals=0,
        ),
        compiler_params=pltpu.CompilerParams(dimension_semantics=("arbitrary",)),
    )(*lefts, near, other)


def arriving(tiles, after=None):
    if after is not None:
        tiles, _ = lax.optimization_barrier((tiles, after))
    return lax.all_to_all(tiles, YZ, 0, 0, tiled=True)


def summed(arrived):
    return jnp.sum(arrived.astype(F32), axis=0)


def owned(own, peer, at_own, core, unit):
    keep, send = chosen(at_own, own, peer), chosen(at_own, peer, own)
    count = keep.shape[0] // 2

    def part(value, index):
        return chosen(index == 0, value[:count], value[count:])

    far = lax.ppermute(part(send, 1 - core), (X, C), ACROSS)
    near = part(keep, core) + exchanged(part(send, core), X)
    far = far + exchanged(part(keep, 1 - core), C)
    rows = in_order(core, near, far, 1)
    dots = jnp.sum(rows * unit, axis=1)
    return rows, (dots + exchanged(dots))[:, None]


def shards(hidden, queries, attn_keys, w_value, w_out, alpha, out_grad):
    rows = w_value.shape[0]
    tokens, width = queries.shape
    heads = width // HS
    side, core, grp = lax.axis_index(X), lax.axis_index(C), lax.axis_index(G)
    at_own = side == grp

    next_v = exchanged(w_value, X)
    pair_v = jnp.stack((chosen(at_own, next_v, w_value), chosen(at_own, w_value, next_v)))
    other_v = exchanged(columns(pair_v, 1 - core), C)
    pair_v = in_order(core, columns(pair_v, core), other_v, 1)
    pieces = spread(pair_v)
    pieces_far = tuple([exchanged(p, C) for p in group] for group in pieces)

    hidden_near, hidden_far = lax.optimization_barrier(
        (columns(hidden, core), columns(hidden, 1 - core))
    )
    raw_near, raw_far, part = placed(pieces, pieces_far, hidden_near, hidden_far)

    next_o = exchanged(w_out, X)
    own_vf, own_of = w_value.astype(F32), w_out.astype(F32)
    next_of = next_o.astype(F32)
    own_part = jnp.stack((jnp.sum(own_of * own_of, axis=1), jnp.sum(own_vf * own_vf, axis=1)))
    next_part = jnp.sum(next_of * next_of, axis=1)
    own_sq = own_part + lax.ppermute(own_part, G, SWAP)
    next_sq = next_part + lax.ppermute(own_part[0], (X, G), ACROSS)
    norm_o, norm_v = jnp.sqrt(own_sq[0] + EPS)[:, None], jnp.sqrt(own_sq[1] + EPS)[:, None]
    unit_v, unit_o = own_vf / norm_v, own_of / norm_o
    here = unit_o.astype(BF16)
    there = (next_of / jnp.sqrt(next_sq + EPS)[:, None]).astype(BF16)
    pair_o = jnp.stack((chosen(at_own, here, there), chosen(at_own, there, here)))
    send_o = columns(pair_o, 1 - core)
    other_o = exchanged(send_o, C)
    pair_o = in_order(core, columns(pair_o, core), other_o, 1)
    both_o = over_planes(pair_o)
    both_o_far = exchanged(both_o, C)
    weight_o = in_order(core, both_o, both_o_far, 3)
    weight_o = weight_o.reshape(2, width, -1)
    weight_o_own, weight_o_peer = weight_o[0], weight_o[1]

    (probs,) = heads_call(
        probs_kernel, heads, ((queries, 0), (attn_keys, 0)), (((heads, tokens, tokens), F32, 0),), 1
    )
    hidden_other = exchanged(hidden_far, C)
    full = (tokens, width)
    value_peer = exchanged(part)
    value_own = contract_last(hidden_near, raw_near[1]) + contract_last(hidden_far, raw_far[1])
    near, far, _ = lax.optimization_barrier((raw_near, raw_far, part))
    half_sq = jnp.sum(jnp.square(near.astype(F32)), axis=2)
    half_sq = half_sq + jnp.sum(jnp.square(far.astype(F32)), axis=2)
    all_sq = half_sq + exchanged(half_sq)[::-1]
    own_rate = jnp.broadcast_to(lax.rsqrt(all_sq[1] + EPS)[None], (8, width))
    values, attn_own = heads_call(
        forward_kernel,
        heads,
        ((probs, 0), (value_own, 0), (value_peer, 0), (own_rate, 0)),
        ((full, BF16, 0), (full, BF16, 0)),
        1,
    )
    attn_their = exchanged(attn_own)
    weight_v = in_order(core, near, far, 2).astype(F32) / jnp.sqrt(all_sq + EPS)[..., None]
    weight_v_peer, weight_v_own = weight_v[0].astype(BF16), weight_v[1].astype(BF16)

    attn_own_other = exchanged(attn_own, C)
    proj = lax.optimization_barrier(matmul(attn_own, weight_o_own))
    attn_their_other = exchanged(attn_their, C)
    proj = proj + matmul(attn_their, weight_o_peer)
    hidden_f = hidden.astype(F32)
    grad_out = out_grad.astype(F32)
    keep_rate = 1.0 - alpha
    moments = jnp.stack(
        (
            jnp.sum(proj * proj, axis=1),
            jnp.sum(keep_rate * keep_rate * hidden_f * hidden_f, axis=1),
            jnp.sum(keep_rate * alpha * hidden_f * proj, axis=1),
            jnp.sum(alpha * alpha * proj * proj, axis=1),
            jnp.sum(grad_out * keep_rate * hidden_f, axis=1),
            jnp.sum(grad_out * alpha * proj, axis=1),
        )
    )
    moments = moments + exchanged(moments)
    proj_rs = lax.rsqrt(moments[0] / D + EPS)[:, None]
    cross_sum = moments[2][:, None]
    alpha_sum = moments[3][:, None]
    mix_mean = (moments[1][:, None] + 2.0 * proj_rs * cross_sum + proj_rs * proj_rs * alpha_sum) / D
    mix_rs = lax.rsqrt(mix_mean + EPS)
    mixed = hidden_f + alpha * (proj * proj_rs - hidden_f)
    new_hidden = (mixed * mix_rs).astype(BF16)
    grad_mean = (moments[4][:, None] + proj_rs * moments[5][:, None]) / D
    grad_mix = mix_rs * (grad_out - mixed * mix_rs * mix_rs * grad_mean)
    grad_pn = grad_mix * alpha
    proj_mean = (
        mix_rs * moments[5][:, None]
        - mix_rs * mix_rs * mix_rs * grad_mean * (cross_sum + proj_rs * alpha_sum)
    ) / D
    grad_res = grad_mix * keep_rate
    grad_proj = proj_rs * (grad_pn - proj * proj_rs * proj_rs * proj_mean)
    grad_proj_b = grad_proj.astype(BF16)

    grad_near, grad_far = lax.optimization_barrier(
        (columns(grad_proj_b, core), columns(grad_proj_b, 1 - core))
    )
    grad_other = exchanged(grad_far, C)
    part = contract_last(grad_proj_b, weight_o_peer).astype(BF16)
    grad_peer = exchanged(part)
    grad_own = contract_last(grad_proj_b, weight_o_own)
    lefts = (attn_own, attn_own_other, attn_their, attn_their_other)
    at_o = arriving(products(lefts, grad_near, grad_other, 2 * rows))
    gw_o = summed(at_o)
    grad_q, grad_k, gv_own = heads_call(
        backward_kernel,
        heads,
        tuple((o, 0) for o in (queries, attn_keys, values, probs, grad_own, grad_peer)),
        ((full, BF16, 0),) * 3,
        4,
    )
    gv_peer = exchanged(gv_own)

    gv_own_other = exchanged(gv_own, C)
    tiles = products((gv_own, gv_own_other), hidden_near, hidden_other, 2 * rows)
    at_own_v = arriving(tiles, at_o)
    gw_v_own = summed(at_own_v)[0]
    gv_peer_other = exchanged(gv_peer, C)
    tiles = products((gv_peer, gv_peer_other), hidden_near, hidden_other, 2 * rows)
    gw_v_peer = summed(arriving(tiles, at_own_v))[0]
    from_own = lax.optimization_barrier(matmul(gv_own, weight_v_own))
    from_peer = lax.optimization_barrier(matmul(gv_peer, weight_v_peer))
    grad_hidden = (grad_res + from_own + from_peer).astype(BF16)
    gw_o_mine, dot_o = owned(gw_o[0], gw_o[1], at_own, core, unit_o)
    gw_v_mine, dot_v = owned(gw_v_own, gw_v_peer, at_own, core, unit_v)
    grad_w_value = (gw_v_mine - unit_v * dot_v) / norm_v
    grad_w_out = (gw_o_mine - unit_o * dot_o) / norm_o
    return new_hidden, grad_hidden, grad_q, grad_k, grad_w_value, grad_w_out


def solution(mesh):
    torus = Mesh(mesh.devices.reshape(2, 4, 4, 2, mesh.shape[G]), (*FSDP, G))
    placed = P(FSDP, G)
    return jax.shard_map(
        shards,
        mesh=torus,
        in_specs=(placed,) * 5 + (P(G), placed),
        out_specs=(placed,) * 6,
        check_vma=False,
    )
```

```python
import functools

import jax
import jax.numpy as jnp
from jax import lax
from jax.experimental import pallas as pl
from jax.experimental.pallas import tpu as pltpu
from jax.sharding import Mesh
from jax.sharding import PartitionSpec as P


D = 3072
HS = 128
X, Y, Z, C, G = "fsdp_0", "fsdp_1", "fsdp_2", "fsdp_3", "grp"
FSDP = (X, Y, Z, C)
YZ = (Y, Z)
EPS = 1e-06
SWAP = [(0, 1), (1, 0)]
ACROSS = [(0, 3), (1, 2), (2, 1), (3, 0)]
F32 = jnp.float32
BF16 = jnp.bfloat16


def contract_last(left, right):
    return lax.dot_general(left, right, (((1,), (1,)), ((), ())), preferred_element_type=F32)


def contract_first(left, right):
    return lax.dot_general(left, right, (((0,), (0,)), ((), ())), preferred_element_type=F32)


def matmul(left, right):
    return jnp.dot(left, right, preferred_element_type=F32)


def causal_halves(length):
    half = length // 2
    return ((0, half), (half, length))


def probs_kernel(q_ref, k_ref, p_ref):
    for lo, hi in causal_halves(q_ref.shape[0]):
        scores = contract_last(q_ref[lo:hi, :], k_ref[:hi, :]) * (HS**-0.5)
        row_pos = lax.broadcasted_iota(jnp.int32, scores.shape, 0) + lo
        col_pos = lax.broadcasted_iota(jnp.int32, scores.shape, 1)
        scores = jnp.where(row_pos >= col_pos, scores, -1e30)
        terms = jnp.exp(scores - jnp.max(scores, axis=1, keepdims=True))
        p_ref[0, lo:hi, :hi] = terms * (1.0 / jnp.sum(terms, axis=1, keepdims=True))


def forward_kernel(p_ref, own_ref, peer_ref, rate_ref, v_ref, attn_ref):
    value = ((own_ref[...] + peer_ref[...].astype(F32)) * rate_ref[0:1, :]).astype(BF16)
    v_ref[...] = value
    for lo, hi in causal_halves(p_ref.shape[1]):
        attn_ref[lo:hi, :] = matmul(p_ref[0, lo:hi, :hi].astype(BF16), value[:hi]).astype(BF16)


def backward_kernel(q_ref, k_ref, v_ref, p_ref, own_ref, peer_ref, dq_ref, dk_ref, dv_ref):
    scale = HS**-0.5
    grad = (own_ref[...] + peer_ref[...].astype(F32)).astype(BF16)
    grad_keys, grad_values = [], []
    for lo, hi in causal_halves(p_ref.shape[1]):
        prob = p_ref[0, lo:hi, :hi]
        grad_prob = contract_last(grad[lo:hi], v_ref[:hi, :])
        delta = jnp.sum(prob * grad_prob, axis=1, keepdims=True)
        grad_score = (prob * (grad_prob - delta)).astype(BF16)
        dq_ref[lo:hi, :] = (matmul(grad_score, k_ref[:hi, :]) * scale).astype(BF16)
        grad_keys.append(contract_first(grad_score, q_ref[lo:hi, :]))
        grad_values.append(contract_first(prob.astype(BF16), grad[lo:hi]))
    half = grad_keys[0].shape[0]
    for out_ref, (early, late), rate in ((dk_ref, grad_keys, scale), (dv_ref, grad_values, 1.0)):
        out_ref[:half, :] = ((early + late[:half]) * rate).astype(BF16)
        out_ref[half:, :] = (late[half:] * rate).astype(BF16)


def heads_call(kernel, heads, operands, results, dots):
    def spec(shape, first):
        if len(shape) == 3:
            return pl.BlockSpec((1, *shape[1:]), lambda h: (first + h, 0, 0))
        return pl.BlockSpec((shape[0], HS), lambda h: (0, first + h))

    tokens = operands[0][0].shape[-2]
    return pl.pallas_call(
        kernel,
        grid=(heads,),
        in_specs=[spec(o.shape, first) for o, first in operands],
        out_specs=[spec(shape, first) for shape, _, first in results],
        out_shape=[jax.ShapeDtypeStruct(shape, dtype) for shape, dtype, _ in results],
        cost_estimate=pl.CostEstimate(
            flops=4 * dots * heads * tokens * tokens * HS,
            bytes_accessed=heads * tokens * (tokens * 4 + HS * 10),
            transcendentals=0,
        ),
        compiler_params=pltpu.CompilerParams(dimension_semantics=("arbitrary",)),
    )(*[o for o, _ in operands])


def exchanged(value, axis=G):
    return lax.ppermute(value, axis, SWAP)


def chosen(first_if, first, second):
    return jnp.where(first_if, first, second)


def columns(value, index):
    half = value.shape[-1] // 2
    return jnp.where(index == 0, value[..., :half], value[..., half:])


def in_order(index, mine, other, axis):
    return jnp.where(
        index == 0,
        jnp.concatenate([mine, other], axis),
        jnp.concatenate([other, mine], axis),
    )


def over_planes(rows):
    planes = lax.axis_size(Y) * lax.axis_size(Z)
    got = lax.all_to_all(jnp.broadcast_to(rows[None], (planes, *rows.shape)), YZ, 0, 0, tiled=True)
    return got.swapaxes(0, 1) if rows.ndim == 3 else got.reshape(-1, rows.shape[-1])


def shifted(value, axis, step):
    count = lax.axis_size(axis)
    return lax.ppermute(value, axis, [(i, (i + step) % count) for i in range(count)])


def spread(rows):
    ny, nz = lax.axis_size(Y), lax.axis_size(Z)
    half = rows.shape[-1] // 2
    left, right = rows[..., :half], rows[..., half:]
    left = jnp.stack([left] + [shifted(left, Y, k) for k in range(1, ny)])
    right = jnp.stack([right] + [shifted(right, Z, k) for k in range(1, nz)])
    lefts = [left] + [shifted(left, Z, k) for k in range(1, nz)]
    rights = [right] + [shifted(right, Y, k) for k in range(1, ny)]
    return lefts, rights


def placed_kernel(place_ref, *refs, ny, nz):
    *pieces, near_ref, far_ref, near_rows, far_rows, part_ref = refs
    each, half = pieces[0].shape[2:]
    y, z = place_ref[0], place_ref[1]

    def run(plane_y, plane_z):
        return pl.ds(pl.multiple_of((plane_y * nz + plane_z) * each, each), each)

    for group, rows_ref in ((0, near_rows), (ny + nz, far_rows)):
        for ky in range(ny):
            for kz in range(nz):
                at = run(lax.rem(y + ny - ky, ny), lax.rem(z + nz - kz, nz))
                for block in range(2):
                    rows_ref[block, at, :half] = pieces[group + kz][ky, block]
                    rows_ref[block, at, half:] = pieces[group + nz + ky][kz, block]
    step = near_ref.shape[0] // 2

    @pl.loop(0, 2)
    def _(i):
        at = pl.ds(pl.multiple_of(i * step, step), step)
        part = contract_last(near_ref[at, :], near_rows[0])
        part = part + contract_last(far_ref[at, :], far_rows[0])
        part_ref[at, :] = part.astype(BF16)


def placed(near, far, hidden_near, hidden_far):
    nz, ny = len(near[0]), len(near[1])
    pieces = (*near[0], *near[1], *far[0], *far[1])
    each, half = pieces[0].shape[2:]
    count = ny * nz * each
    tokens = hidden_near.shape[0]
    place = jnp.stack((lax.axis_index(Y), lax.axis_index(Z))).astype(jnp.int32)
    vmem = pl.BlockSpec(memory_space=pltpu.VMEM)
    rows = jax.ShapeDtypeStruct((2, count, 2 * half), BF16)
    return pl.pallas_call(
        functools.partial(placed_kernel, ny=ny, nz=nz),
        in_specs=[pl.BlockSpec(memory_space=pltpu.SMEM)] + [vmem] * (len(pieces) + 2),
        out_specs=[vmem] * 3,
        out_shape=[rows, rows, jax.ShapeDtypeStruct((tokens, count), BF16)],
        cost_estimate=pl.CostEstimate(
            flops=8 * tokens * count * half, bytes_accessed=16 * count * half, transcendentals=0
        ),
    )(place, *pieces, hidden_near, hidden_far)


def product_kernel(*refs):
    *lefts, near_ref, other_ref, out_ref = refs
    runs, _, each, width = out_ref.shape
    for i in range(len(lefts) // 2):
        total = contract_first(lefts[2 * i][...], near_ref[...])
        total = total + contract_first(lefts[2 * i + 1][...], other_ref[...])
        out_ref[:, i] = total.astype(BF16).reshape(runs, each, width)


def products(lefts, near, other, each, steps=2):
    tokens, count = lefts[0].shape
    width = near.shape[1]
    block = count // steps
    pairs = len(lefts) // 2
    return pl.pallas_call(
        product_kernel,
        grid=(steps,),
        in_specs=[pl.BlockSpec((tokens, block), lambda i: (0, i))] * len(lefts)
        + [pl.BlockSpec((tokens, width), lambda i: (0, 0))] * 2,
        out_specs=pl.BlockSpec((block // each, pairs, each, width), lambda i: (i, 0, 0, 0)),
        out_shape=jax.ShapeDtypeStruct((count // each, pairs, each, width), BF16),
        cost_estimate=pl.CostEstimate(
            flops=2 * tokens * count * width * len(lefts),
            bytes_accessed=4 * count * width,
            transcendentals=0,
        ),
        compiler_params=pltpu.CompilerParams(dimension_semantics=("arbitrary",)),
    )(*lefts, near, other)


def arriving(tiles, after=None):
    if after is not None:
        tiles, _ = lax.optimization_barrier((tiles, after))
    return lax.all_to_all(tiles, YZ, 0, 0, tiled=True)


def summed(arrived):
    return jnp.sum(arrived.astype(F32), axis=0)


def owned(own, peer, at_own, core, unit):
    keep, send = chosen(at_own, own, peer), chosen(at_own, peer, own)
    count = keep.shape[0] // 2

    def part(value, index):
        return chosen(index == 0, value[:count], value[count:])

    far = lax.ppermute(part(send, 1 - core), (X, C), ACROSS)
    near = part(keep, core) + exchanged(part(send, core), X)
    far = far + exchanged(part(keep, 1 - core), C)
    rows = in_order(core, near, far, 1)
    dots = jnp.sum(rows * unit, axis=1)
    return rows, (dots + exchanged(dots))[:, None]


def shards(hidden, queries, attn_keys, w_value, w_out, alpha, out_grad):
    rows = w_value.shape[0]
    tokens, width = queries.shape
    heads = width // HS
    side, core, grp = lax.axis_index(X), lax.axis_index(C), lax.axis_index(G)
    at_own = side == grp

    next_v = exchanged(w_value, X)
    pair_v = jnp.stack((chosen(at_own, next_v, w_value), chosen(at_own, w_value, next_v)))
    other_v = exchanged(columns(pair_v, 1 - core), C)
    pair_v = in_order(core, columns(pair_v, core), other_v, 1)
    pieces = spread(pair_v)
    pieces_far = tuple([exchanged(p, C) for p in group] for group in pieces)

    hidden_near, hidden_far = lax.optimization_barrier(
        (columns(hidden, core), columns(hidden, 1 - core))
    )
    raw_near, raw_far, part = placed(pieces, pieces_far, hidden_near, hidden_far)

    next_o = exchanged(w_out, X)
    own_vf, own_of = w_value.astype(F32), w_out.astype(F32)
    next_of = next_o.astype(F32)
    own_part = jnp.stack((jnp.sum(own_of * own_of, axis=1), jnp.sum(own_vf * own_vf, axis=1)))
    next_part = jnp.sum(next_of * next_of, axis=1)
    own_sq = own_part + lax.ppermute(own_part, G, SWAP)
    next_sq = next_part + lax.ppermute(own_part[0], (X, G), ACROSS)
    norm_o, norm_v = jnp.sqrt(own_sq[0] + EPS)[:, None], jnp.sqrt(own_sq[1] + EPS)[:, None]
    unit_v, unit_o = own_vf / norm_v, own_of / norm_o
    here = unit_o.astype(BF16)
    there = (next_of / jnp.sqrt(next_sq + EPS)[:, None]).astype(BF16)
    pair_o = jnp.stack((chosen(at_own, here, there), chosen(at_own, there, here)))
    send_o = columns(pair_o, 1 - core)
    other_o = exchanged(send_o, C)
    pair_o = in_order(core, columns(pair_o, core), other_o, 1)
    both_o = over_planes(pair_o)
    both_o_far = exchanged(both_o, C)
    weight_o = in_order(core, both_o, both_o_far, 3)
    weight_o = weight_o.reshape(2, width, -1)
    weight_o_own, weight_o_peer = weight_o[0], weight_o[1]

    (probs,) = heads_call(
        probs_kernel, heads, ((queries, 0), (attn_keys, 0)), (((heads, tokens, tokens), F32, 0),), 1
    )
    hidden_other = exchanged(hidden_far, C)
    full = (tokens, width)
    value_peer = exchanged(part)
    value_own = contract_last(hidden_near, raw_near[1]) + contract_last(hidden_far, raw_far[1])
    near, far, _ = lax.optimization_barrier((raw_near, raw_far, part))
    half_sq = jnp.sum(jnp.square(near.astype(F32)), axis=2)
    half_sq = half_sq + jnp.sum(jnp.square(far.astype(F32)), axis=2)
    all_sq = half_sq + exchanged(half_sq)[::-1]
    own_rate = jnp.broadcast_to(lax.rsqrt(all_sq[1] + EPS)[None], (8, width))
    values, attn_own = heads_call(
        forward_kernel,
        heads,
        ((probs, 0), (value_own, 0), (value_peer, 0), (own_rate, 0)),
        ((full, BF16, 0), (full, BF16, 0)),
        1,
    )
    attn_their = exchanged(attn_own)
    weight_v = in_order(core, near, far, 2).astype(F32) / jnp.sqrt(all_sq + EPS)[..., None]
    weight_v_peer, weight_v_own = weight_v[0].astype(BF16), weight_v[1].astype(BF16)

    attn_own_other = exchanged(attn_own, C)
    proj = lax.optimization_barrier(matmul(attn_own, weight_o_own))
    attn_their_other = exchanged(attn_their, C)
    proj = proj + matmul(attn_their, weight_o_peer)
    hidden_f = hidden.astype(F32)
    grad_out = out_grad.astype(F32)
    keep_rate = 1.0 - alpha
    moments = jnp.stack(
        (
            jnp.sum(proj * proj, axis=1),
            jnp.sum(keep_rate * keep_rate * hidden_f * hidden_f, axis=1),
            jnp.sum(keep_rate * alpha * hidden_f * proj, axis=1),
            jnp.sum(alpha * alpha * proj * proj, axis=1),
            jnp.sum(grad_out * keep_rate * hidden_f, axis=1),
            jnp.sum(grad_out * alpha * proj, axis=1),
        )
    )
    moments = moments + exchanged(moments)
    proj_rs = lax.rsqrt(moments[0] / D + EPS)[:, None]
    cross_sum = moments[2][:, None]
    alpha_sum = moments[3][:, None]
    mix_mean = (moments[1][:, None] + 2.0 * proj_rs * cross_sum + proj_rs * proj_rs * alpha_sum) / D
    mix_rs = lax.rsqrt(mix_mean + EPS)
    mixed = hidden_f + alpha * (proj * proj_rs - hidden_f)
    new_hidden = (mixed * mix_rs).astype(BF16)
    grad_mean = (moments[4][:, None] + proj_rs * moments[5][:, None]) / D
    grad_mix = mix_rs * (grad_out - mixed * mix_rs * mix_rs * grad_mean)
    grad_pn = grad_mix * alpha
    proj_mean = (
        mix_rs * moments[5][:, None]
        - mix_rs * mix_rs * mix_rs * grad_mean * (cross_sum + proj_rs * alpha_sum)
    ) / D
    grad_res = grad_mix * keep_rate
    grad_proj = proj_rs * (grad_pn - proj * proj_rs * proj_rs * proj_mean)
    grad_proj_b = grad_proj.astype(BF16)

    grad_near, grad_far = lax.optimization_barrier(
        (columns(grad_proj_b, core), columns(grad_proj_b, 1 - core))
    )
    grad_other = exchanged(grad_far, C)
    part = contract_last(grad_proj_b, weight_o_peer).astype(BF16)
    grad_peer = exchanged(part)
    grad_own = contract_last(grad_proj_b, weight_o_own)
    lefts = (attn_own, attn_own_other, attn_their, attn_their_other)
    at_o = arriving(products(lefts, grad_near, grad_other, 2 * rows))
    gw_o = summed(at_o)
    grad_q, grad_k, gv_own = heads_call(
        backward_kernel,
        heads,
        tuple((o, 0) for o in (queries, attn_keys, values, probs, grad_own, grad_peer)),
        ((full, BF16, 0),) * 3,
        4,
    )
    gv_peer = exchanged(gv_own)

    gv_own_other = exchanged(gv_own, C)
    tiles = products((gv_own, gv_own_other), hidden_near, hidden_other, 2 * rows)
    at_own_v = arriving(tiles, at_o)
    gw_v_own = summed(at_own_v)[0]
    gv_peer_other = exchanged(gv_peer, C)
    tiles = products((gv_peer, gv_peer_other), hidden_near, hidden_other, 2 * rows)
    gw_v_peer = summed(arriving(tiles, at_own_v))[0]
    from_own = lax.optimization_barrier(matmul(gv_own, weight_v_own))
    from_peer = lax.optimization_barrier(matmul(gv_peer, weight_v_peer))
    grad_hidden = (grad_res + from_own + from_peer).astype(BF16)
    gw_o_mine, dot_o = owned(gw_o[0], gw_o[1], at_own, core, unit_o)
    gw_v_mine, dot_v = owned(gw_v_own, gw_v_peer, at_own, core, unit_v)
    grad_w_value = (gw_v_mine - unit_v * dot_v) / norm_v
    grad_w_out = (gw_o_mine - unit_o * dot_o) / norm_o
    return new_hidden, grad_hidden, grad_q, grad_k, grad_w_value, grad_w_out


def solution(mesh):
    torus = Mesh(mesh.devices.reshape(2, 4, 4, 2, mesh.shape[G]), (*FSDP, G))
    placed = P(FSDP, G)
    return jax.shard_map(
        shards,
        mesh=torus,
        in_specs=(placed,) * 5 + (P(G), placed),
        out_specs=(placed,) * 6,
        check_vma=False,
    )
```
